8 devices in a mesh: dp: 1 (over z), tp: 2 (over y), ep: 4 (over x, core).
Axes of the slice: x: 2, y: 2, z: 1, core: 2. Of those that a mesh axis runs over, the one named last changes fastest.
Arguments:
- resid_in: bfloat16 [512, 2048], P(('dp', 'ep'))
- norm_scale: bfloat16 [2048], replicated
- w_router: bfloat16 [2048, 128], replicated
- w_gate: bfloat16 [128, 2048, 768], P('ep', None, 'tp')
- w_up: bfloat16 [128, 2048, 768], P('ep', None, 'tp')
- w_down: bfloat16 [128, 768, 2048], P('ep', 'tp')
- choice: int32 [512, 8], P(('dp', 'ep'))
Outputs:
- output: bfloat16 [512, 2048], P(('dp', 'ep'))
All inputs are finite; a program needn't handle non-finite values.
Results may differ from the reference program's by a relative error of at most 0.00530799.
Values are sent between devices in bfloat16 or wider.
A program may use at most 1 GiB of HBM per device.

```python
import jax
import jax.numpy as jnp
from jax import lax

D_MODEL = 2048
EXPERTS = 128
TOP_K = 8
TOK_DEV = 128
FF_SHARD = 384
EP_GROUPS = 4
TP_SHARDS = 2

TOKENS = EP_GROUPS * TOK_DEV
FF_WIDTH = TP_SHARDS * FF_SHARD
CAPACITY = (2 * TOK_DEV * TOP_K + EXPERTS - 1) // EXPERTS
NUM_SLOTS = EXPERTS * EP_GROUPS * CAPACITY
NORM_EPS = 1e-5


def draw_choice(choice_key):
    base_key, bias_key = jax.random.split(choice_key)
    base_score = jax.random.randint(base_key, (TOKENS, EXPERTS), 0, 65536, dtype=jnp.int32)
    expert_bias = jax.random.randint(bias_key, (EXPERTS,), 0, 16384, dtype=jnp.int32)
    scores = (base_score + expert_bias[None, :]) * EXPERTS + jnp.arange(EXPERTS, dtype=jnp.int32)[None, :]
    return lax.top_k(scores, TOP_K)[1].astype(jnp.int32)


def setup_inputs(seed: int = 0, part: int = 0) -> dict:
    root_key = jax.random.key(seed)
    sub_keys = jax.random.split(root_key, 7)
    resid_in = jax.random.normal(jax.random.fold_in(sub_keys[0], part), (TOKENS, D_MODEL), jnp.float32)
    norm_scale = 1.0 + 0.3 * jax.random.normal(sub_keys[1], (D_MODEL,), jnp.float32)
    w_router = jax.random.normal(sub_keys[2], (D_MODEL, EXPERTS), jnp.float32) * D_MODEL ** -0.5
    w_gate = jax.random.normal(sub_keys[3], (EXPERTS, D_MODEL, FF_WIDTH), jnp.float32) * D_MODEL ** -0.5
    w_up = jax.random.normal(sub_keys[4], (EXPERTS, D_MODEL, FF_WIDTH), jnp.float32) * D_MODEL ** -0.5
    w_down = jax.random.normal(sub_keys[5], (EXPERTS, FF_WIDTH, D_MODEL), jnp.float32) * (2.0 * FF_WIDTH ** -0.5)
    choice = draw_choice(jax.random.fold_in(sub_keys[6], part))
    return {'resid_in': resid_in.astype(jnp.bfloat16), 'norm_scale': norm_scale.astype(jnp.bfloat16), 'w_router': w_router.astype(jnp.bfloat16), 'w_gate': w_gate.astype(jnp.bfloat16), 'w_up': w_up.astype(jnp.bfloat16), 'w_down': w_down.astype(jnp.bfloat16), 'choice': choice}


def norm_route(resid_rows, norm_scale, w_router, choice_rows):
    rows_f32 = resid_rows.astype(jnp.float32)
    centered = rows_f32 - jnp.mean(rows_f32, axis=-1, keepdims=True)
    variance = jnp.mean(centered * centered, axis=-1, keepdims=True)
    normed = (centered * lax.rsqrt(variance + NORM_EPS) * norm_scale.astype(jnp.float32)).astype(jnp.bfloat16)
    logits = jnp.dot(normed, w_router, preferred_element_type=jnp.float32)
    router_probs = jax.nn.softmax(logits, axis=-1)
    expert_ids = jnp.arange(w_router.shape[1], dtype=jnp.int32)
    picked = jnp.sum(jnp.where(choice_rows[:, :, None] == expert_ids[None, None, :], router_probs[:, None, :], 0.0), axis=-1)
    gate_vals = picked / jnp.sum(picked, axis=-1, keepdims=True)
    return normed, gate_vals


def expert_glu(rows_in, w_gate_e, w_up_e, w_down_e):
    gate_act = jnp.dot(rows_in, w_gate_e, preferred_element_type=jnp.float32)
    up_act = jnp.dot(rows_in, w_up_e, preferred_element_type=jnp.float32)
    hidden = (jax.nn.silu(gate_act) * up_act).astype(jnp.bfloat16)
    hidden_split = hidden.reshape(rows_in.shape[0], TP_SHARDS, FF_SHARD).astype(jnp.float32)
    down_split = w_down_e.reshape(TP_SHARDS, FF_SHARD, D_MODEL).astype(jnp.float32)
    partial_out = jnp.einsum('stf,tfd->tsd', hidden_split, down_split).astype(jnp.bfloat16)
    return jnp.sum(partial_out.astype(jnp.float32), axis=0)


def reference(resid_in, norm_scale, w_router, w_gate, w_up, w_down, choice):
    normed, gate_vals = norm_route(resid_in, norm_scale, w_router, choice)
    group_choice = choice.reshape(EP_GROUPS, TOK_DEV * TOP_K)
    onehot = (group_choice[:, :, None] == jnp.arange(EXPERTS, dtype=jnp.int32)[None, None, :]).astype(jnp.int32)
    earlier = jnp.cumsum(onehot, axis=1) - onehot
    position = jnp.sum(earlier * onehot, axis=2)
    is_kept = (position < CAPACITY).reshape(-1)
    group_ids = jnp.arange(EP_GROUPS, dtype=jnp.int32)[:, None]
    slot_ids = (group_choice * (EP_GROUPS * CAPACITY) + group_ids * CAPACITY + position).reshape(-1)
    target = jnp.where(is_kept, slot_ids, NUM_SLOTS)
    token_rows = (group_ids * TOK_DEV + jnp.arange(TOK_DEV * TOP_K, dtype=jnp.int32)[None, :] // TOP_K).reshape(-1)
    source_row = jnp.zeros((NUM_SLOTS + 1,), jnp.int32).at[target].set(token_rows)[:NUM_SLOTS]
    kept_gate = jnp.where(is_kept, gate_vals.reshape(-1), 0.0)
    slot_gate = jnp.zeros((NUM_SLOTS + 1,), jnp.float32).at[target].set(kept_gate)[:NUM_SLOTS]

    def expert_step(mixed_sum, expert_in):
        rows_idx, gate_col, w_gate_e, w_up_e, w_down_e = expert_in
        y_rows = expert_glu(normed[rows_idx], w_gate_e, w_up_e, w_down_e)
        return mixed_sum.at[rows_idx].add(gate_col[:, None] * y_rows), None

    mixed_sum, unused = lax.scan(expert_step, jnp.zeros((TOKENS, D_MODEL), jnp.float32), (source_row.reshape(EXPERTS, EP_GROUPS * CAPACITY), slot_gate.reshape(EXPERTS, EP_GROUPS * CAPACITY), w_gate, w_up, w_down))
    return (resid_in.astype(jnp.float32) + mixed_sum).astype(jnp.bfloat16)
```

```python
import functools

import jax
import jax.numpy as jnp
from jax import lax
from jax.experimental import pallas as pl
from jax.experimental.pallas import tpu as pltpu
from jax.sharding import PartitionSpec as P

NORM_EPS = 1e-5
MESH = pl.DeviceIdType.MESH
F32 = jnp.float32
BF16 = jnp.bfloat16

SLOTS = 12
HEAD_CHUNKS = 4
LAG_X = 1
LAG_Y = 3
LAG_OUT = 5


def moe_kernel(dims, x_hbm, scale_hbm, router_hbm, gate_hbm, up_hbm, down_hbm, choice_hbm, out_hbm,
               ring, xall, uall, xbatch, hid, disp, comb, qbuf, part, pair_in, row_in, col_in, out_v,
               scale_v, router_v, choice_t, ring_sem, ring_sem2, load_sem, pair_send, pair_recv, fwd_send, fwd_recv,
               hop_send, hop_recv, ch_send, ch_recv, p_send, p_recv, x_send, x_recv, y_send, y_recv, out_sem):
    tok, d_model, experts, top_k, local, width, groups, cap, cols = dims
    chunks = d_model // cols
    gate_fills, half = local, local // 2
    fills = gate_fills + 2 * chunks
    per_row = (2 * width) // cols
    ep = lax.axis_index('ep')
    tp = lax.axis_index('tp')
    dp = lax.axis_index('dp')
    sib = ep + 1 - 2 * (ep % 2)
    opp = (ep + 2) % 4
    diag = (sib + 2) % 4
    to_sib, to_opp, to_tp = (dp, tp, sib), (dp, tp, opp), (dp, 1 - tp, ep)

    def gate_copies(f, slot):
        return (pltpu.make_async_copy(gate_hbm.at[f], ring.at[slot, pl.ds(0, d_model), pl.ds(0, width)], ring_sem.at[slot]),
                pltpu.make_async_copy(up_hbm.at[f], ring.at[slot, pl.ds(0, d_model), pl.ds(width, width)], ring_sem.at[slot]))

    def down_place(i):
        return (i // per_row) * width, (i % per_row) * cols

    def start_fill(f, slot):
        @pl.when(f < gate_fills)
        def _():
            for copy in gate_copies(f, slot):
                copy.start()

        @pl.when(jnp.logical_and(f >= gate_fills, f < fills))
        def _():
            h = f - gate_fills
            c, base = h // 2, (h % 2) * half
            col = pl.multiple_of(c * cols, cols)
            for i in range(half):
                row, lane = down_place(i)
                sem = ring_sem if i < half - 1 else ring_sem2
                pltpu.make_async_copy(down_hbm.at[base + i, :, pl.ds(col, cols)],
                                      ring.at[slot, pl.ds(row, width), pl.ds(lane, cols)], sem.at[slot]).start()

    def wait_gate(slot):
        view = ring.at[slot, pl.ds(0, d_model), :]
        pltpu.make_async_copy(view, view, ring_sem.at[slot]).wait()

    def wait_down(slot):
        rows = ((half - 1) // per_row) * width
        view = ring.at[slot, pl.ds(0, rows), :]
        pltpu.make_async_copy(view, view, ring_sem.at[slot]).wait()
        row, lane = down_place(half - 1)
        view = ring.at[slot, pl.ds(row, width), pl.ds(lane, cols)]
        pltpu.make_async_copy(view, view, ring_sem2.at[slot]).wait()

    own_x = pltpu.make_async_copy(x_hbm, xall.at[ep], load_sem.at[0])
    own_choice = pltpu.make_async_copy(choice_hbm, choice_t.at[ep], load_sem.at[1])
    own_scale = pltpu.make_async_copy(scale_hbm, scale_v, load_sem.at[2])
    own_router = pltpu.make_async_copy(router_hbm, router_v, load_sem.at[3])
    own_choice.start()
    own_x.start()
    own_scale.start()

    barrier = pltpu.get_barrier_semaphore()
    for peer in (to_sib, to_opp, to_tp):
        pl.semaphore_signal(barrier, inc=1, device_id=peer, device_id_type=MESH)
    for f in range(4):
        for copy in gate_copies(f, f):
            copy.start()
    own_router.start()
    pl.semaphore_wait(barrier, 3)

    def remote(src, dst, ssem, rsem, peer):
        return pltpu.make_async_remote_copy(src_ref=src, dst_ref=dst, send_sem=ssem, recv_sem=rsem, device_id=peer, device_id_type=MESH)

    piece = tok // HEAD_CHUNKS
    to_pair = remote(x_hbm, xall.at[ep], pair_send, pair_recv, to_sib)
    hops = [remote(x_hbm.at[pl.ds(r * piece, piece), :], xall.at[ep, pl.ds(r * piece, piece), :], hop_send.at[r], hop_recv.at[r], to_opp)
            for r in range(HEAD_CHUNKS)]
    forwards = [remote(xall.at[opp, pl.ds(r * piece, piece), :], xall.at[opp, pl.ds(r * piece, piece), :], fwd_send.at[r], fwd_recv.at[r], to_sib)
                for r in range(HEAD_CHUNKS)]
    ch_pair = remote(choice_hbm, choice_t.at[ep], ch_send.at[0], ch_recv.at[0], to_sib)
    ch_hop = remote(choice_hbm, choice_t.at[ep], ch_send.at[1], ch_recv.at[1], to_opp)
    ch_fwd = remote(choice_t.at[opp], choice_t.at[opp], ch_send.at[2], ch_recv.at[2], to_sib)
    ch_hop.start()
    ch_pair.start()
    hops[0].start()
    to_pair.start()

    for r in range(1, HEAD_CHUNKS):
        hops[r].start()

    @pl.loop(4, SLOTS)
    def _(f):
        start_fill(f, f)

    row_e = lax.broadcasted_iota(jnp.int32, (experts, tok), 0)
    earlier = (lax.broadcasted_iota(jnp.int32, (tok, tok), 0) < lax.broadcasted_iota(jnp.int32, (tok, tok), 1)).astype(BF16)
    slots = local * cap
    slot_row = lax.broadcasted_iota(jnp.int32, (slots, experts), 0)
    expand_t = (lax.broadcasted_iota(jnp.int32, (slots, experts), 1) == ep * local + slot_row // cap).astype(BF16)
    slot_col = lax.broadcasted_iota(jnp.int32, (experts, slots), 1)
    expand = (lax.broadcasted_iota(jnp.int32, (experts, slots), 0) == ep * local + slot_col // cap).astype(BF16)
    cap_row = (lax.broadcasted_iota(jnp.int32, (slots, tok), 0) % cap).astype(F32)
    cap_col = (lax.broadcasted_iota(jnp.int32, (tok, slots), 1) % cap).astype(F32)

    def positions(g):
        ids = choice_t[g]
        member = jnp.zeros((experts, tok), F32)
        for k in range(top_k):
            member = jnp.where(row_e == ids[k:k + 1, :], 1.0, member)
        before = jnp.dot(member.astype(BF16), earlier, preferred_element_type=F32)
        return member, jnp.where(member > 0.0, before, 255.0)

    def dispatch_table(g):
        member, place = positions(g)
        spot = jnp.dot(expand_t, place.astype(BF16), preferred_element_type=F32)
        disp[g] = (spot == cap_row).astype(BF16)

    def combine_table(g):
        member, place = positions(g)
        logits = jnp.dot(uall[g], router_v[...], preferred_element_type=F32)
        shifted = jnp.exp(logits - jnp.max(logits, axis=-1, keepdims=True))
        probs = shifted / jnp.sum(shifted, axis=-1, keepdims=True)
        picked = jnp.where(jnp.transpose(member) > 0.0, probs, 0.0)
        gates = picked / jnp.sum(picked, axis=-1, keepdims=True)
        spot = jnp.dot(jnp.transpose(place).astype(BF16), expand, preferred_element_type=F32)
        filled = spot == cap_col
        rest = gates
        for i in range(3):
            term = rest.astype(BF16)
            rest = rest - term.astype(F32)
            wide = jnp.dot(term, expand, preferred_element_type=F32)
            comb[g, pl.ds(i * tok, tok), :] = jnp.where(filled, wide, 0.0).astype(BF16)

    def normalize(g):
        n = d_model // 128
        scale = scale_v[...].astype(F32)
        total = jnp.zeros((tok, 128), F32)
        for j in range(n):
            total = total + xall[g, :, pl.ds(j * 128, 128)].astype(F32)
        mean = jnp.sum(total, axis=-1, keepdims=True) / d_model
        square = jnp.zeros((tok, 128), F32)
        for j in range(n):
            centered = xall[g, :, pl.ds(j * 128, 128)].astype(F32) - mean
            square = square + centered * centered
        inv = lax.rsqrt(jnp.sum(square, axis=-1, keepdims=True) / d_model + NORM_EPS)
        for j in range(n):
            centered = xall[g, :, pl.ds(j * 128, 128)].astype(F32) - mean
            uall[g, :, pl.ds(j * 128, 128)] = (centered * inv * scale[j:j + 1, :]).astype(BF16)

    own_choice.wait()
    own_scale.wait()
    own_x.wait()
    dispatch_table(ep)
    normalize(ep)
    ch_pair.wait_recv()
    dispatch_table(sib)
    to_pair.wait_recv()
    normalize(sib)
    for r in range(HEAD_CHUNKS):
        hops[r].wait_recv()
        forwards[r].start()
        if r == 0:
            ch_hop.wait_recv()
            ch_fwd.start()
            dispatch_table(opp)
            ch_fwd.wait_recv()
            dispatch_table(diag)
    normalize(opp)
    for r in range(HEAD_CHUNKS):
        forwards[r].wait_recv()
    normalize(diag)
    own_router.wait()

    batch = tok // cap
    wide = 512

    @pl.loop(0, local // batch)
    def _(b):
        for g in range(groups):
            table = disp[g, pl.ds(pl.multiple_of(b * tok, tok), tok), :]
            for j in range(d_model // wide):
                xbatch[g, :, pl.ds(j * wide, wide)] = jnp.dot(table, uall[g, :, pl.ds(j * wide, wide)], preferred_element_type=F32).astype(BF16)
        combine_table(b)

        @pl.loop(0, batch)
        def _(i):
            e = b * batch + i
            slot = e % SLOTS
            wait_gate(slot)
            row = pl.multiple_of(i * cap, cap)
            rows = jnp.concatenate([xbatch[g, pl.ds(row, cap), :] for g in range(groups)], axis=0)
            both = jnp.dot(rows, ring[slot, pl.ds(0, d_model), :], preferred_element_type=F32)
            hid[e] = (jax.nn.silu(both[:, :width]) * both[:, width:]).astype(BF16)
            start_fill(e + SLOTS, slot)

    mine, theirs = ep, opp

    def pair_copy(c, j):
        return remote(part.at[c, (1 - ep % 2) + 2 * j], pair_in.at[c, j], p_send.at[c, j], p_recv.at[c, j], to_sib)

    def x_copy(c):
        return remote(part.at[c, theirs], row_in.at[c], x_send.at[c], x_recv.at[c], to_opp)

    def y_copy(c):
        return remote(part.at[c, mine], col_in.at[c], y_send.at[c], y_recv.at[c], to_tp)

    def out_copy(c):
        col = pl.multiple_of(c * cols, cols)
        return pltpu.make_async_copy(out_v.at[:, pl.ds(col, cols)], out_hbm.at[:, pl.ds(col, cols)], out_sem.at[c])

    def compute(c):
        for h in range(2):
            f = gate_fills + 2 * c + h
            slot = f % SLOTS
            wait_down(slot)
            for i in range(half):
                row, lane = down_place(i)
                e = h * half + i
                q = jnp.dot(hid[e], ring[slot, pl.ds(row, width), pl.ds(lane, cols)], preferred_element_type=F32).astype(BF16)
                for g in range(groups):
                    qbuf[g, pl.ds(e * cap, cap), :] = q[g * cap:(g + 1) * cap, :]
            start_fill(f + SLOTS, slot)
        for g in range(groups):
            terms = jnp.dot(comb[g], qbuf[g], preferred_element_type=F32)
            part[c, g] = terms[0:tok] + terms[tok:2 * tok] + terms[2 * tok:3 * tok]
        for j in range(2):
            pair_copy(c, j).start()

    def send_x(c):
        far = 1 - ep // 2
        pair_copy(c, far).wait_recv()
        part[c, theirs] = part[c, theirs] + pair_in[c, far]
        x_copy(c).start()
        pair_copy(c, 1 - far).wait_recv()
        part[c, mine] = part[c, mine] + pair_in[c, 1 - far]

    def send_y(c):
        x_copy(c).wait_recv()
        part[c, mine] = part[c, mine] + row_in[c]
        y_copy(c).start()

    def finish(c):
        y_copy(c).wait_recv()
        col = pl.multiple_of(c * cols, cols)
        total = part[c, mine] + col_in[c]
        out_v[:, pl.ds(col, cols)] = (xall[ep, :, pl.ds(col, cols)].astype(F32) + total).astype(BF16)
        out_copy(c).start()

    @pl.loop(0, chunks + LAG_OUT)
    def _(c):
        @pl.when(c < chunks)
        def _():
            compute(c)

        for lag, stage in ((LAG_X, send_x), (LAG_Y, send_y), (LAG_OUT, finish)):
            @pl.when(jnp.logical_and(c >= lag, c < chunks + lag))
            def _():
                stage(c - lag)

    to_pair.wait_send()
    for r in range(HEAD_CHUNKS):
        hops[r].wait_send()
        forwards[r].wait_send()
    ch_pair.wait_send()
    ch_hop.wait_send()
    ch_fwd.wait_send()

    @pl.loop(0, chunks)
    def _(c):
        for j in range(2):
            pair_copy(c, j).wait_send()
        x_copy(c).wait_send()
        y_copy(c).wait_send()
        out_copy(c).wait()


def solution(mesh):
    row_spec = P(('dp', 'ep'), None)

    def device_step(resid_in, norm_scale, w_router, w_gate, w_up, w_down, choice):
        tok, d_model = resid_in.shape
        experts, top_k = w_router.shape[1], choice.shape[1]
        local, width = w_gate.shape[0], w_gate.shape[2]
        groups = experts // local
        cap = (2 * tok * top_k + experts - 1) // experts
        cols = 256
        chunks = d_model // cols
        dims = (tok, d_model, experts, top_k, local, width, groups, cap, cols)
        dma = pltpu.SemaphoreType.DMA
        vmem = pltpu.VMEM
        return pl.pallas_call(
            functools.partial(moe_kernel, dims),
            out_shape=jax.ShapeDtypeStruct((tok, d_model), BF16),
            in_specs=[pl.BlockSpec(memory_space=pl.ANY)] * 7,
            out_specs=pl.BlockSpec(memory_space=pl.ANY),
            scratch_shapes=[
                vmem((SLOTS, 6 * width, 2 * width), BF16),
                vmem((groups, tok, d_model), BF16),
                vmem((groups, tok, d_model), BF16),
                vmem((groups, tok, d_model), BF16),
                vmem((local, groups * cap, width), BF16),
                vmem((groups, local * cap, tok), BF16),
                vmem((groups, 3 * tok, local * cap), BF16),
                vmem((groups, local * cap, cols), BF16),
                vmem((chunks, groups, tok, cols), F32),
                vmem((chunks, 2, tok, cols), F32),
                vmem((chunks, tok, cols), F32),
                vmem((chunks, tok, cols), F32),
                vmem((tok, d_model), BF16),
                vmem((d_model // 128, 128), BF16),
                vmem((d_model, experts), BF16),
                vmem((groups, top_k, tok), jnp.int32),
                dma((SLOTS,)), dma((SLOTS,)), dma((4,)),
                dma(()), dma(()), dma((HEAD_CHUNKS,)), dma((HEAD_CHUNKS,)), dma((HEAD_CHUNKS,)), dma((HEAD_CHUNKS,)),
                dma((3,)), dma((3,)),
                dma((chunks, 2)), dma((chunks, 2)), dma((chunks,)), dma((chunks,)), dma((chunks,)), dma((chunks,)), dma((chunks,)),
            ],
            compiler_params=pltpu.CompilerParams(collective_id=0, has_side_effects=True, vmem_limit_bytes=67043328),
        )(resid_in, norm_scale.reshape(d_model // 128, 128), w_router, w_gate, w_up, w_down, choice.T)

    return jax.shard_map(device_step, mesh=mesh, in_specs=(row_spec, P(None), P(None, None), P('ep', None, 'tp'), P('ep', None, 'tp'), P('ep', 'tp', None), row_spec), out_specs=row_spec, check_vma=False)
```

```python
import functools

import jax
import jax.numpy as jnp
from jax import lax
from jax.experimental import pallas as pl
from jax.experimental.pallas import tpu as pltpu
from jax.sharding import PartitionSpec as P

NORM_EPS = 1e-5
MESH = pl.DeviceIdType.MESH
F32 = jnp.float32
BF16 = jnp.bfloat16

SLOTS = 14
PAIR_SLOTS = 4
UNROLL = 4
HEAD_CHUNKS = 4
LAG_X = 1
LAG_Y = 3
LAG_OUT = 5


def moe_kernel(dims, x_hbm, scale_hbm, router_hbm, gate_hbm, up_hbm, down_hbm, choice_hbm, out_hbm,
               ring, xall, uall, xbatch, hid, disp, comb, qbuf, part, pair_out, pair_in, row_in, col_in,
               scale_v, router_v, choice_t, ring_sem, load_sem, pair_send, pair_recv, hop_send, hop_recv, tp_send, tp_recv,
               near_send, near_recv, far_send, far_recv, ch_send, ch_recv, p_send, p_recv, x_send, x_recv, y_send, y_recv, out_sem):
    tok, d_model, experts, top_k, local, width, groups, cap, cols = dims
    chunks = d_model // cols
    half = local // 2
    fills = local + 2 * chunks
    ep = lax.axis_index('ep')
    tp = lax.axis_index('tp')
    dp = lax.axis_index('dp')
    core, side = ep % 2, ep // 2
    sib = ep + 1 - 2 * core
    opp = (ep + 2) % 4
    diag = (sib + 2) % 4
    to_sib, to_opp, to_tp = (dp, tp, sib), (dp, tp, opp), (dp, 1 - tp, ep)

    def gate_copies(f, slot):
        return (pltpu.make_async_copy(gate_hbm.at[f], ring.at[slot, :, pl.ds(0, width)], ring_sem.at[slot]),
                pltpu.make_async_copy(up_hbm.at[f], ring.at[slot, :, pl.ds(width, width)], ring_sem.at[slot]))

    def down_pieces(i):
        pieces, done = [], 0
        while done < width:
            at = i * width + done
            rows = min(width - done, d_model - at % d_model)
            pieces.append((done, rows, at % d_model, (at // d_model) * cols))
            done += rows
        return pieces

    def start_fill(f, slot):
        @pl.when(f < local)
        def _():
            for copy in gate_copies(f, slot):
                copy.start()

        @pl.when(jnp.logical_and(f >= local, f < fills))
        def _():
            h = f - local
            c, base = h // 2, (h % 2) * half
            col = pl.multiple_of(c * cols, cols)
            for i in range(half):
                for begin, rows, row, lane in down_pieces(i):
                    pltpu.make_async_copy(down_hbm.at[base + i, pl.ds(begin, rows), pl.ds(col, cols)],
                                          ring.at[slot, pl.ds(row, rows), pl.ds(lane, cols)], ring_sem.at[slot]).start()

    def wait_fill(slot):
        pltpu.make_async_copy(ring.at[slot], ring.at[slot], ring_sem.at[slot]).wait()

    own_x = pltpu.make_async_copy(x_hbm, xall.at[ep], load_sem.at[0])
    own_choice = pltpu.make_async_copy(choice_hbm, choice_t.at[ep], load_sem.at[1])
    own_scale = pltpu.make_async_copy(scale_hbm, scale_v, load_sem.at[2])
    own_router = pltpu.make_async_copy(router_hbm, router_v, load_sem.at[3])
    own_x.start()
    own_choice.start()
    own_scale.start()
    own_router.start()

    barrier = pltpu.get_barrier_semaphore()
    for peer in (to_sib, to_opp, to_tp):
        pl.semaphore_signal(barrier, inc=1, device_id=peer, device_id_type=MESH)
    for f in range(SLOTS):
        for copy in gate_copies(f, f):
            copy.start()

    def remote(src, dst, ssem, rsem, peer):
        return pltpu.make_async_remote_copy(src_ref=src, dst_ref=dst, send_sem=ssem, recv_sem=rsem, device_id=peer, device_id_type=MESH)

    mid = tok // 2
    piece = mid // HEAD_CHUNKS

    def rows_of(which, r):
        return pl.ds(pl.multiple_of(which * mid + r * piece, piece), piece)

    def same(block, rows, ssem, rsem, peer):
        return remote(xall.at[block, rows, :], xall.at[block, rows, :], ssem, rsem, peer)

    span = range(HEAD_CHUNKS)
    to_pair = remote(xall.at[ep], xall.at[ep], pair_send, pair_recv, to_sib)
    hops = [same(ep, rows_of(tp, r), hop_send.at[r], hop_recv.at[r], to_opp) for r in span]
    over = [same(opp, rows_of(tp, r), tp_send.at[r], tp_recv.at[r], to_tp) for r in span]
    near = [same(opp, rows_of(tp, r), near_send.at[r], near_recv.at[r], to_sib) for r in span]
    far = [same(opp, rows_of(1 - tp, r), far_send.at[r], far_recv.at[r], to_sib) for r in span]
    ch_pair = remote(choice_t.at[ep], choice_t.at[ep], ch_send.at[0], ch_recv.at[0], to_sib)
    ch_hop = remote(choice_t.at[ep], choice_t.at[ep], ch_send.at[1], ch_recv.at[1], to_opp)
    ch_fwd = remote(choice_t.at[opp], choice_t.at[opp], ch_send.at[2], ch_recv.at[2], to_sib)
    own_choice.wait()
    own_x.wait()
    pl.semaphore_wait(barrier, 3)
    ch_hop.start()
    for r in span:
        hops[r].start()
    ch_pair.start()
    to_pair.start()

    row_e = lax.broadcasted_iota(jnp.int32, (experts, tok), 0)
    earlier = (lax.broadcasted_iota(jnp.int32, (tok, tok), 0) < lax.broadcasted_iota(jnp.int32, (tok, tok), 1)).astype(BF16)
    slots = local * cap
    slot_row = lax.broadcasted_iota(jnp.int32, (slots, experts), 0)
    expand_t = (lax.broadcasted_iota(jnp.int32, (slots, experts), 1) == ep * local + slot_row // cap).astype(BF16)
    slot_col = lax.broadcasted_iota(jnp.int32, (experts, slots), 1)
    expand = (lax.broadcasted_iota(jnp.int32, (experts, slots), 0) == ep * local + slot_col // cap).astype(BF16)
    cap_row = (lax.broadcasted_iota(jnp.int32, (slots, tok), 0) % cap).astype(F32)
    cap_col = (lax.broadcasted_iota(jnp.int32, (tok, slots), 1) % cap).astype(F32)

    def positions(g):
        ids = choice_t[g]
        member = jnp.zeros((experts, tok), F32)
        for k in range(top_k):
            member = jnp.where(row_e == ids[k:k + 1, :], 1.0, member)
        before = jnp.dot(member.astype(BF16), earlier, preferred_element_type=F32)
        return member, jnp.where(member > 0.0, before, 255.0)

    def dispatch_table(g):
        member, place = positions(g)
        spot = jnp.dot(expand_t, place.astype(BF16), preferred_element_type=F32)
        disp[g] = (spot == cap_row).astype(BF16)

    def combine_table(g):
        member, place = positions(g)
        logits = jnp.dot(uall[g], router_v[...], preferred_element_type=F32)
        shifted = jnp.exp(logits - jnp.max(logits, axis=-1, keepdims=True))
        probs = shifted / jnp.sum(shifted, axis=-1, keepdims=True)
        picked = jnp.where(jnp.transpose(member) > 0.0, probs, 0.0)
        gates = picked / jnp.sum(picked, axis=-1, keepdims=True)
        spot = jnp.dot(jnp.transpose(place).astype(BF16), expand, preferred_element_type=F32)
        filled = spot == cap_col
        rest = gates
        for i in range(3):
            term = rest.astype(BF16)
            rest = rest - term.astype(F32)
            wide = jnp.dot(term, expand, preferred_element_type=F32)
            comb[g, pl.ds(i * tok, tok), :] = jnp.where(filled, wide, 0.0).astype(BF16)

    def normalize(g, first, rows):
        n = d_model // 128
        at = pl.ds(first, rows)
        scale = scale_v[...].astype(F32)
        total = jnp.zeros((rows, 128), F32)
        for j in range(n):
            total = total + xall[g, at, pl.ds(j * 128, 128)].astype(F32)
        mean = jnp.sum(total, axis=-1, keepdims=True) / d_model
        square = jnp.zeros((rows, 128), F32)
        for j in range(n):
            centered = xall[g, at, pl.ds(j * 128, 128)].astype(F32) - mean
            square = square + centered * centered
        inv = lax.rsqrt(jnp.sum(square, axis=-1, keepdims=True) / d_model + NORM_EPS)
        for j in range(n):
            centered = xall[g, at, pl.ds(j * 128, 128)].astype(F32) - mean
            uall[g, at, pl.ds(j * 128, 128)] = (centered * inv * scale[j:j + 1, :]).astype(BF16)

    here, there = pl.multiple_of(tp * mid, mid), pl.multiple_of((1 - tp) * mid, mid)
    own_scale.wait()
    normalize(ep, 0, tok)
    dispatch_table(ep)
    ch_pair.wait_recv()
    to_pair.wait_recv()
    normalize(sib, 0, tok)
    dispatch_table(sib)
    own_router.wait()
    combine_table(ep)

    def pass_hop(r):
        hops[r].wait_recv()
        over[r].start()
        near[r].start()

    def pass_over(r):
        over[r].wait_recv()
        far[r].start()

    ch_hop.wait_recv()
    ch_fwd.start()
    lead = 2
    for r in range(lead):
        pass_hop(r)
    combine_table(sib)
    dispatch_table(opp)
    ch_fwd.wait_recv()
    dispatch_table(diag)
    for r in range(lead, HEAD_CHUNKS):
        pass_hop(r)
        pass_over(r - lead)
    normalize(opp, here, mid)
    for r in range(HEAD_CHUNKS - lead, HEAD_CHUNKS):
        pass_over(r)
    for r in span:
        near[r].wait_recv()
    normalize(diag, here, mid)
    normalize(opp, there, mid)
    for r in span:
        far[r].wait_recv()
    normalize(diag, there, mid)

    batch = tok // cap
    wide = 512

    @pl.loop(0, local // batch)
    def _(b):
        for g in range(groups):
            table = disp[g, pl.ds(pl.multiple_of(b * tok, tok), tok), :]
            for j in range(d_model // wide):
                xbatch[g, :, pl.ds(j * wide, wide)] = jnp.dot(table, uall[g, :, pl.ds(j * wide, wide)], preferred_element_type=F32).astype(BF16)

        @pl.when(jnp.logical_and(b >= 1, b < 3))
        def _():
            combine_table(jnp.where(b == 1, opp, diag))

        @pl.loop(0, batch // UNROLL)
        def _(i):
            first = b * batch + i * UNROLL
            for k in range(UNROLL):
                wait_fill((first + k) % SLOTS)
            for k in range(UNROLL):
                row = pl.multiple_of((i * UNROLL + k) * cap, cap)
                rows = jnp.concatenate([xbatch[g, pl.ds(row, cap), :] for g in range(groups)], axis=0)
                both = jnp.dot(rows, ring[(first + k) % SLOTS], preferred_element_type=F32)
                hid[first + k] = (jax.nn.silu(both[:, :width]) * both[:, width:]).astype(BF16)
            for k in range(UNROLL):
                start_fill(first + k + SLOTS, (first + k) % SLOTS)

    def pair_copy(c, j):
        return remote(pair_out.at[c % PAIR_SLOTS, j], pair_in.at[c, j], p_send.at[c, j], p_recv.at[c, j], to_sib)

    def at_cols(c):
        return pl.ds(pl.multiple_of(c * cols, cols), cols)

    def x_copy(c):
        return remote(xbatch.at[0, :, at_cols(c)], row_in.at[:, at_cols(c)], x_send.at[c], x_recv.at[c], to_opp)

    def y_copy(c):
        return remote(xbatch.at[1, :, at_cols(c)], col_in.at[:, at_cols(c)], y_send.at[c], y_recv.at[c], to_tp)

    def out_copy(c):
        return pltpu.make_async_copy(xbatch.at[2, :, at_cols(c)], out_hbm.at[:, at_cols(c)], out_sem.at[c])

    def half_products(c, h):
        f = local + 2 * c + h
        slot = f % SLOTS
        wait_fill(slot)
        for i in range(half):
            e = h * half + i
            parts = [ring[slot, pl.ds(row, rows), pl.ds(lane, cols)] for begin, rows, row, lane in down_pieces(i)]
            weight = parts[0] if len(parts) == 1 else jnp.concatenate(parts, axis=0)
            q = jnp.dot(hid[e], weight, preferred_element_type=F32).astype(BF16)
            for g in range(groups):
                qbuf[g, pl.ds(e * cap, cap), :] = q[g * cap:(g + 1) * cap, :]
        start_fill(f + SLOTS, slot)

    def weighted(g):
        terms = jnp.dot(comb[g], qbuf[g], preferred_element_type=F32)
        return terms[0:tok] + terms[tok:2 * tok] + terms[2 * tok:3 * tok]

    def sums(c):
        @pl.when(c >= PAIR_SLOTS)
        def _():
            for j in range(2):
                pair_copy(c - PAIR_SLOTS, j).wait_send()

        for j in range(2):
            pair_out[c % PAIR_SLOTS, j] = weighted(2 * j + 1 - core)
            pair_copy(c, j).start()
        for j in range(2):
            part[c, j] = weighted(2 * j + core)

    def send_x(c):
        for j in range(2):
            pair_copy(c, j).wait_recv()
        xbatch[0, :, at_cols(c)] = (part[c, 1 - side] + pair_in[c, 1 - side]).astype(BF16)
        x_copy(c).start()
        part[c, side] = part[c, side] + pair_in[c, side]

    def send_y(c):
        x_copy(c).wait_recv()
        xbatch[1, :, at_cols(c)] = (part[c, side] + row_in[:, at_cols(c)].astype(F32)).astype(BF16)
        y_copy(c).start()

    def finish(c):
        y_copy(c).wait_recv()
        total = xbatch[1, :, at_cols(c)].astype(F32) + col_in[:, at_cols(c)].astype(F32)
        xbatch[2, :, at_cols(c)] = (xall[ep, :, at_cols(c)].astype(F32) + total).astype(BF16)
        out_copy(c).start()

    @pl.loop(0, chunks + LAG_OUT)
    def _(c):
        @pl.when(c < chunks)
        def _():
            half_products(c, 0)

        for lag, stage in ((LAG_X, send_x), (LAG_Y, send_y), (LAG_OUT, finish)):
            @pl.when(jnp.logical_and(c >= lag, c < chunks + lag))
            def _():
                stage(c - lag)

        @pl.when(c < chunks)
        def _():
            half_products(c, 1)
            sums(c)

    to_pair.wait_send()
    for copies in (hops, over, near, far):
        for r in span:
            copies[r].wait_send()
    ch_pair.wait_send()
    ch_hop.wait_send()
    ch_fwd.wait_send()

    @pl.loop(chunks - PAIR_SLOTS, chunks)
    def _(c):
        for j in range(2):
            pair_copy(c, j).wait_send()

    @pl.loop(0, chunks)
    def _(c):
        x_copy(c).wait_send()
        y_copy(c).wait_send()
        out_copy(c).wait()


def solution(mesh):
    row_spec = P(('dp', 'ep'), None)

    def device_step(resid_in, norm_scale, w_router, w_gate, w_up, w_down, choice):
        tok, d_model = resid_in.shape
        experts, top_k = w_router.shape[1], choice.shape[1]
        local, width = w_gate.shape[0], w_gate.shape[2]
        groups = experts // local
        cap = (2 * tok * top_k + experts - 1) // experts
        cols = 256
        chunks = d_model // cols
        dims = (tok, d_model, experts, top_k, local, width, groups, cap, cols)
        dma = pltpu.SemaphoreType.DMA
        vmem = pltpu.VMEM
        return pl.pallas_call(
            functools.partial(moe_kernel, dims),
            out_shape=jax.ShapeDtypeStruct((tok, d_model), BF16),
            in_specs=[pl.BlockSpec(memory_space=pl.ANY)] * 7,
            out_specs=pl.BlockSpec(memory_space=pl.ANY),
            scratch_shapes=[
                vmem((SLOTS, d_model, 2 * width), BF16),
                vmem((groups, tok, d_model), BF16),
                vmem((groups, tok, d_model), BF16),
                vmem((groups, tok, d_model), BF16),
                vmem((local, groups * cap, width), BF16),
                vmem((groups, local * cap, tok), BF16),
                vmem((groups, 3 * tok, local * cap), BF16),
                vmem((groups, local * cap, cols), BF16),
                vmem((chunks, 2, tok, cols), F32),
                vmem((PAIR_SLOTS, 2, tok, cols), F32),
                vmem((chunks, 2, tok, cols), F32),
                vmem((tok, d_model), BF16),
                vmem((tok, d_model), BF16),
                vmem((d_model // 128, 128), BF16),
                vmem((d_model, experts), BF16),
                vmem((groups, top_k, tok), jnp.int32),
                dma((SLOTS,)), dma((4,)), dma(()), dma(()),
                *[dma((HEAD_CHUNKS,)) for _ in range(8)],
                dma((3,)), dma((3,)),
                dma((chunks, 2)), dma((chunks, 2)),
                *[dma((chunks,)) for _ in range(5)],
            ],
            compiler_params=pltpu.CompilerParams(collective_id=0, has_side_effects=True, vmem_limit_bytes=67043328),
        )(resid_in, norm_scale.reshape(d_model // 128, 128), w_router, w_gate, w_up, w_down, choice.T)

    return jax.shard_map(device_step, mesh=mesh, in_specs=(row_spec, P(None), P(None, None), P('ep', None, 'tp'), P('ep', None, 'tp'), P('ep', 'tp', None), row_spec), out_specs=row_spec, check_vma=False)
```

```python
import functools

import jax
import jax.numpy as jnp
from jax import lax
from jax.experimental import pallas as pl
from jax.experimental.pallas import tpu as pltpu
from jax.sharding import PartitionSpec as P

NORM_EPS = 1e-5
MESH = pl.DeviceIdType.MESH
F32 = jnp.float32
BF16 = jnp.bfloat16

SLOTS = 14
PAIR_SLOTS = 4
UNROLL = 4
HEAD_CHUNKS = 4
LAG_X = 1
LAG_Y = 3
LAG_OUT = 5


def moe_kernel(dims, x_hbm, scale_hbm, router_hbm, gate_hbm, up_hbm, down_hbm, choice_hbm, out_hbm,
               ring, xall, uall, xbatch, hid, disp, comb, qbuf, part, pair_out, pair_in, row_in, col_in,
               scale_v, router_v, choice_t, ring_sem, load_sem, pair_send, pair_recv, hop_send, hop_recv, tp_send, tp_recv,
               near_send, near_recv, far_send, far_recv, ch_send, ch_recv, p_send, p_recv, x_send, x_recv, y_send, y_recv, out_sem):
    tok, d_model, experts, top_k, local, width, groups, cap, cols = dims
    chunks = d_model // cols
    half = local // 2
    fills = local + 2 * chunks
    ep = lax.axis_index('ep')
    tp = lax.axis_index('tp')
    dp = lax.axis_index('dp')
    core, side = ep % 2, ep // 2
    sib = ep + 1 - 2 * core
    opp = (ep + 2) % 4
    diag = (sib + 2) % 4
    to_sib, to_opp, to_tp = (dp, tp, sib), (dp, tp, opp), (dp, 1 - tp, ep)

    lane_tiles = width // 128
    row_tiles = d_model // 128
    side_tiles = cols // 128
    per_expert = width // 128

    def start_gate(f, slot):
        for n, source in enumerate((gate_hbm, up_hbm)):
            for j in range(lane_tiles):
                pltpu.make_async_copy(source.at[f, :, :, pl.ds(j * 128, 128)], ring.at[slot, n * lane_tiles + j], ring_sem.at[slot]).start()

    def start_fill(f, slot):
        @pl.when(f < local)
        def _():
            start_gate(f, slot)

        @pl.when(jnp.logical_and(f >= local, f < fills))
        def _():
            h = f - local
            col = (h // 2) * cols
            base = (h % 2) * half * per_expert
            for b in range(2 * lane_tiles):
                lane = pl.multiple_of(col + (b // lane_tiles) * 128, 128)
                pltpu.make_async_copy(down_hbm.at[pl.ds(base + (b % lane_tiles) * row_tiles, row_tiles), :, pl.ds(lane, 128)],
                                      ring.at[slot, b], ring_sem.at[slot]).start()

    def wait_fill(slot):
        pltpu.make_async_copy(ring.at[slot], ring.at[slot], ring_sem.at[slot]).wait()

    own_x = pltpu.make_async_copy(x_hbm, xall.at[ep], load_sem.at[0])
    own_choice = pltpu.make_async_copy(choice_hbm, choice_t.at[ep], load_sem.at[1])
    own_scale = pltpu.make_async_copy(scale_hbm, scale_v, load_sem.at[2])
    own_router = pltpu.make_async_copy(router_hbm, router_v, load_sem.at[3])
    own_x.start()
    own_choice.start()
    own_scale.start()
    own_router.start()

    barrier = pltpu.get_barrier_semaphore()
    for peer in (to_sib, to_opp, to_tp):
        pl.semaphore_signal(barrier, inc=1, device_id=peer, device_id_type=MESH)
    for f in range(SLOTS):
        start_gate(f, f)

    def remote(src, dst, ssem, rsem, peer):
        return pltpu.make_async_remote_copy(src_ref=src, dst_ref=dst, send_sem=ssem, recv_sem=rsem, device_id=peer, device_id_type=MESH)

    mid = tok // 2
    piece = mid // HEAD_CHUNKS

    def rows_of(which, r):
        return pl.ds(pl.multiple_of(which * mid + r * piece, piece), piece)

    def same(block, rows, ssem, rsem, peer):
        return remote(xall.at[block, rows, :], xall.at[block, rows, :], ssem, rsem, peer)

    span = range(HEAD_CHUNKS)
    to_pair = remote(xall.at[ep], xall.at[ep], pair_send, pair_recv, to_sib)
    hops = [same(ep, rows_of(tp, r), hop_send.at[r], hop_recv.at[r], to_opp) for r in span]
    over = [same(opp, rows_of(tp, r), tp_send.at[r], tp_recv.at[r], to_tp) for r in span]
    near = [same(opp, rows_of(tp, r), near_send.at[r], near_recv.at[r], to_sib) for r in span]
    far = [same(opp, rows_of(1 - tp, r), far_send.at[r], far_recv.at[r], to_sib) for r in span]
    ch_pair = remote(choice_t.at[ep], choice_t.at[ep], ch_send.at[0], ch_recv.at[0], to_sib)
    ch_hop = remote(choice_t.at[ep], choice_t.at[ep], ch_send.at[1], ch_recv.at[1], to_opp)
    ch_fwd = remote(choice_t.at[opp], choice_t.at[opp], ch_send.at[2], ch_recv.at[2], to_sib)
    own_choice.wait()
    own_x.wait()
    pl.semaphore_wait(barrier, 3)
    ch_hop.start()
    for r in span:
        hops[r].start()
    ch_pair.start()
    to_pair.start()

    row_e = lax.broadcasted_iota(jnp.int32, (experts, tok), 0)
    earlier = (lax.broadcasted_iota(jnp.int32, (tok, tok), 0) < lax.broadcasted_iota(jnp.int32, (tok, tok), 1)).astype(BF16)
    slots = local * cap
    slot_row = lax.broadcasted_iota(jnp.int32, (slots, experts), 0)
    expand_t = (lax.broadcasted_iota(jnp.int32, (slots, experts), 1) == ep * local + slot_row // cap).astype(BF16)
    slot_col = lax.broadcasted_iota(jnp.int32, (experts, slots), 1)
    expand = (lax.broadcasted_iota(jnp.int32, (experts, slots), 0) == ep * local + slot_col // cap).astype(BF16)
    cap_row = (lax.broadcasted_iota(jnp.int32, (slots, tok), 0) % cap).astype(F32)
    cap_col = (lax.broadcasted_iota(jnp.int32, (tok, slots), 1) % cap).astype(F32)

    def positions(g):
        ids = choice_t[g]
        member = jnp.zeros((experts, tok), F32)
        for k in range(top_k):
            member = jnp.where(row_e == ids[k:k + 1, :], 1.0, member)
        before = jnp.dot(member.astype(BF16), earlier, preferred_element_type=F32)
        return member, jnp.where(member > 0.0, before, 255.0)

    def dispatch_table(g):
        member, place = positions(g)
        spot = jnp.dot(expand_t, place.astype(BF16), preferred_element_type=F32)
        disp[g] = (spot == cap_row).astype(BF16)

    def combine_table(g):
        member, place = positions(g)
        rows = jnp.concatenate([uall[g, j] for j in range(row_tiles)], axis=1)
        logits = jnp.dot(rows, router_v[...], preferred_element_type=F32)
        shifted = jnp.exp(logits - jnp.max(logits, axis=-1, keepdims=True))
        probs = shifted / jnp.sum(shifted, axis=-1, keepdims=True)
        picked = jnp.where(jnp.transpose(member) > 0.0, probs, 0.0)
        gates = picked / jnp.sum(picked, axis=-1, keepdims=True)
        spot = jnp.dot(jnp.transpose(place).astype(BF16), expand, preferred_element_type=F32)
        filled = spot == cap_col
        rest = gates
        for i in range(3):
            term = rest.astype(BF16)
            rest = rest - term.astype(F32)
            wide = jnp.dot(term, expand, preferred_element_type=F32)
            picked = jnp.where(filled, wide, 0.0).astype(BF16)
            for j in range(slots // 128):
                comb[g, j, pl.ds(i * tok, tok), :] = picked[:, j * 128:(j + 1) * 128]

    def normalize(g, first, rows):
        n = d_model // 128
        at = pl.ds(first, rows)
        scale = scale_v[...].astype(F32)
        total = jnp.zeros((rows, 128), F32)
        for j in range(n):
            total = total + xall[g, at, pl.ds(j * 128, 128)].astype(F32)
        mean = jnp.sum(total, axis=-1, keepdims=True) / d_model
        square = jnp.zeros((rows, 128), F32)
        for j in range(n):
            centered = xall[g, at, pl.ds(j * 128, 128)].astype(F32) - mean
            square = square + centered * centered
        inv = lax.rsqrt(jnp.sum(square, axis=-1, keepdims=True) / d_model + NORM_EPS)
        for j in range(n):
            centered = xall[g, at, pl.ds(j * 128, 128)].astype(F32) - mean
            uall[g, j, at, :] = (centered * inv * scale[j:j + 1, :]).astype(BF16)

    here, there = pl.multiple_of(tp * mid, mid), pl.multiple_of((1 - tp) * mid, mid)
    own_scale.wait()
    normalize(ep, 0, tok)
    dispatch_table(ep)
    ch_pair.wait_recv()
    to_pair.wait_recv()
    normalize(sib, 0, tok)
    dispatch_table(sib)
    own_router.wait()
    combine_table(ep)

    def pass_hop(r):
        hops[r].wait_recv()
        over[r].start()
        near[r].start()

    def pass_over(r):
        over[r].wait_recv()
        far[r].start()

    ch_hop.wait_recv()
    ch_fwd.start()
    lead = 2
    for r in range(lead):
        pass_hop(r)
    combine_table(sib)
    dispatch_table(opp)
    ch_fwd.wait_recv()
    dispatch_table(diag)
    for r in range(lead, HEAD_CHUNKS):
        pass_hop(r)
        pass_over(r - lead)
    normalize(opp, here, mid)
    for r in range(HEAD_CHUNKS - lead, HEAD_CHUNKS):
        pass_over(r)
    for r in span:
        near[r].wait_recv()
    normalize(diag, here, mid)
    normalize(opp, there, mid)
    for r in span:
        far[r].wait_recv()
    normalize(diag, there, mid)

    batch = tok // cap
    group = 4

    @pl.loop(0, local // batch)
    def _(b):
        for g in range(groups):
            table = disp[g, pl.ds(pl.multiple_of(b * tok, tok), tok), :]
            for j in range(0, row_tiles, group):
                block = jnp.concatenate([uall[g, j + t] for t in range(group)], axis=1)
                chosen = jnp.dot(table, block, preferred_element_type=F32).astype(BF16)
                for t in range(group):
                    xbatch[g, j + t] = chosen[:, t * 128:(t + 1) * 128]

        @pl.when(jnp.logical_and(b >= 1, b < 3))
        def _():
            combine_table(jnp.where(b == 1, opp, diag))

        @pl.loop(0, batch // UNROLL)
        def _(i):
            first = b * batch + i * UNROLL
            for k in range(UNROLL):
                wait_fill((first + k) % SLOTS)
            for k in range(UNROLL):
                row = pl.multiple_of((i * UNROLL + k) * cap, cap)
                slot = (first + k) % SLOTS
                rows = jnp.concatenate([jnp.concatenate([xbatch[g, j, pl.ds(row, cap), :] for g in range(groups)], axis=0)
                                        for j in range(row_tiles)], axis=1)
                weight = jnp.concatenate([ring[slot, j].reshape(d_model, 128) for j in range(2 * lane_tiles)], axis=1)
                both = jnp.dot(rows, weight, preferred_element_type=F32)
                hidden = (jax.nn.silu(both[:, :width]) * both[:, width:]).astype(BF16)
                for j in range(lane_tiles):
                    hid[first + k, j] = hidden[:, j * 128:(j + 1) * 128]
            for k in range(UNROLL):
                start_fill(first + k + SLOTS, (first + k) % SLOTS)

    def pair_copy(c, j):
        return remote(pair_out.at[c % PAIR_SLOTS, j], pair_in.at[c, j], p_send.at[c, j], p_recv.at[c, j], to_sib)

    def at_cols(c):
        return pl.ds(pl.multiple_of(c * cols, cols), cols)

    def at_tiles(c):
        return pl.ds(c * side_tiles, side_tiles)

    def x_copy(c):
        return remote(xbatch.at[0, at_tiles(c)], row_in.at[at_tiles(c)], x_send.at[c], x_recv.at[c], to_opp)

    def y_copy(c):
        return remote(xbatch.at[1, at_tiles(c)], col_in.at[at_tiles(c)], y_send.at[c], y_recv.at[c], to_tp)

    def out_copies(c):
        return [pltpu.make_async_copy(xbatch.at[2, c * side_tiles + t],
                                      out_hbm.at[:, pl.ds(pl.multiple_of(c * cols + t * 128, 128), 128)], out_sem.at[c, t])
                for t in range(side_tiles)]

    def half_products(c, h):
        f = local + 2 * c + h
        slot = f % SLOTS
        wait_fill(slot)
        for i in range(half):
            e = h * half + i
            weight = jnp.concatenate([
                jnp.concatenate([ring[slot, a * lane_tiles + (per_expert * i + t) // row_tiles, (per_expert * i + t) % row_tiles]
                                 for t in range(per_expert)], axis=0) for a in range(side_tiles)], axis=1)
            hidden = jnp.concatenate([hid[e, j] for j in range(lane_tiles)], axis=1)
            q = jnp.dot(hidden, weight, preferred_element_type=F32).astype(BF16)
            for g in range(groups):
                for a in range(side_tiles):
                    qbuf[g, a, pl.ds(e * cap, cap), :] = q[g * cap:(g + 1) * cap, a * 128:(a + 1) * 128]
        start_fill(f + SLOTS, slot)

    def weighted(g):
        gates = jnp.concatenate([comb[g, j] for j in range(slots // 128)], axis=1)
        rows = jnp.concatenate([qbuf[g, a] for a in range(side_tiles)], axis=1)
        terms = jnp.dot(gates, rows, preferred_element_type=F32)
        return terms[0:tok] + terms[tok:2 * tok] + terms[2 * tok:3 * tok]

    def sums(c):
        @pl.when(c >= PAIR_SLOTS)
        def _():
            for j in range(2):
                pair_copy(c - PAIR_SLOTS, j).wait_send()

        for j in range(2):
            pair_out[c % PAIR_SLOTS, j] = weighted(2 * j + 1 - core)
            pair_copy(c, j).start()
        for j in range(2):
            part[c, j] = weighted(2 * j + core)

    def send_x(c):
        for j in range(2):
            pair_copy(c, j).wait_recv()
        for t in range(side_tiles):
            at = pl.ds(t * 128, 128)
            xbatch[0, c * side_tiles + t] = (part[c, 1 - side, :, at] + pair_in[c, 1 - side, :, at]).astype(BF16)
        x_copy(c).start()
        part[c, side] = part[c, side] + pair_in[c, side]

    def send_y(c):
        x_copy(c).wait_recv()
        for t in range(side_tiles):
            tile = c * side_tiles + t
            xbatch[1, tile] = (part[c, side, :, pl.ds(t * 128, 128)] + row_in[tile].astype(F32)).astype(BF16)
        y_copy(c).start()

    def finish(c):
        y_copy(c).wait_recv()
        for t in range(side_tiles):
            tile = c * side_tiles + t
            total = xbatch[1, tile].astype(F32) + col_in[tile].astype(F32)
            resid = xall[ep, :, pl.ds(pl.multiple_of(tile * 128, 128), 128)].astype(F32)
            xbatch[2, tile] = (resid + total).astype(BF16)
        for copy in out_copies(c):
            copy.start()

    @pl.loop(0, chunks + LAG_OUT)
    def _(c):
        @pl.when(c < chunks)
        def _():
            half_products(c, 0)
            half_products(c, 1)

        for lag, stage in ((LAG_X, send_x), (LAG_Y, send_y), (LAG_OUT, finish)):
            @pl.when(jnp.logical_and(c >= lag, c < chunks + lag))
            def _():
                stage(c - lag)

        @pl.when(c < chunks)
        def _():
            sums(c)

    to_pair.wait_send()
    for copies in (hops, over, near, far):
        for r in span:
            copies[r].wait_send()
    ch_pair.wait_send()
    ch_hop.wait_send()
    ch_fwd.wait_send()

    @pl.loop(chunks - PAIR_SLOTS, chunks)
    def _(c):
        for j in range(2):
            pair_copy(c, j).wait_send()

    @pl.loop(0, chunks)
    def _(c):
        x_copy(c).wait_send()
        y_copy(c).wait_send()
        for copy in out_copies(c):
            copy.wait()


def solution(mesh):
    row_spec = P(('dp', 'ep'), None)

    def device_step(resid_in, norm_scale, w_router, w_gate, w_up, w_down, choice):
        tok, d_model = resid_in.shape
        experts, top_k = w_router.shape[1], choice.shape[1]
        local, width = w_gate.shape[0], w_gate.shape[2]
        groups = experts // local
        cap = (2 * tok * top_k + experts - 1) // experts
        cols = 256
        chunks = d_model // cols
        dims = (tok, d_model, experts, top_k, local, width, groups, cap, cols)
        dma = pltpu.SemaphoreType.DMA
        vmem = pltpu.VMEM
        return pl.pallas_call(
            functools.partial(moe_kernel, dims),
            out_shape=jax.ShapeDtypeStruct((tok, d_model), BF16),
            in_specs=[pl.BlockSpec(memory_space=pl.ANY)] * 7,
            out_specs=pl.BlockSpec(memory_space=pl.ANY),
            scratch_shapes=[
                vmem((SLOTS, 2 * width // 128, d_model // 128, 128, 128), BF16),
                vmem((groups, tok, d_model), BF16),
                vmem((groups, d_model // 128, tok, 128), BF16),
                vmem((groups, d_model // 128, tok, 128), BF16),
                vmem((local, width // 128, groups * cap, 128), BF16),
                vmem((groups, local * cap, tok), BF16),
                vmem((groups, local * cap // 128, 3 * tok, 128), BF16),
                vmem((groups, cols // 128, local * cap, 128), BF16),
                vmem((chunks, 2, tok, cols), F32),
                vmem((PAIR_SLOTS, 2, tok, cols), F32),
                vmem((chunks, 2, tok, cols), F32),
                vmem((d_model // 128, tok, 128), BF16),
                vmem((d_model // 128, tok, 128), BF16),
                vmem((d_model // 128, 128), BF16),
                vmem((d_model, experts), BF16),
                vmem((groups, top_k, tok), jnp.int32),
                dma((SLOTS,)), dma((4,)), dma(()), dma(()),
                *[dma((HEAD_CHUNKS,)) for _ in range(8)],
                dma((3,)), dma((3,)),
                dma((chunks, 2)), dma((chunks, 2)),
                *[dma((chunks,)) for _ in range(4)],
                dma((chunks, cols // 128)),
            ],
            compiler_params=pltpu.CompilerParams(collective_id=0, has_side_effects=True, vmem_limit_bytes=67043328),
        )(resid_in, norm_scale.reshape(d_model // 128, 128), w_router, w_gate.reshape(local, d_model // 128, 128, width),
          w_up.reshape(local, d_model // 128, 128, width), w_down.reshape(local * width // 128, 128, d_model), choice.T)

    return jax.shard_map(device_step, mesh=mesh, in_specs=(row_spec, P(None), P(None, None), P('ep', None, 'tp'), P('ep', None, 'tp'), P('ep', 'tp', None), row_spec), out_specs=row_spec, check_vma=False)
```

```python
import functools

import jax
import jax.numpy as jnp
from jax import lax
from jax.experimental import pallas as pl
from jax.experimental.pallas import tpu as pltpu
from jax.sharding import PartitionSpec as P

NORM_EPS = 1e-5
MESH = pl.DeviceIdType.MESH
F32 = jnp.float32
BF16 = jnp.bfloat16

SLOTS = 14
PAIR_SLOTS = 4
UNROLL = 4
HEAD_CHUNKS = 8
LAG_X = 1
LAG_Y = 3
LAG_OUT = 5


def moe_kernel(dims, x_hbm, scale_hbm, router_hbm, gate_hbm, up_hbm, down_hbm, choice_hbm, out_hbm,
               ring, xall, uall, xbatch, hid, disp, comb, qbuf, part, pair_out, pair_in, row_in, col_in,
               scale_v, router_v, choice_t, ring_sem, load_sem, pair_send, pair_recv, hop_send, hop_recv, tp_send, tp_recv,
               near_send, near_recv, far_send, far_recv, ch_send, ch_recv, p_send, p_recv, x_send, x_recv, y_send, y_recv, out_sem):
    tok, d_model, experts, top_k, local, width, groups, cap, cols = dims
    chunks = d_model // cols
    half = local // 2
    fills = local + 2 * chunks
    ep = lax.axis_index('ep')
    tp = lax.axis_index('tp')
    dp = lax.axis_index('dp')
    core, side = ep % 2, ep // 2
    sib = ep + 1 - 2 * core
    opp = (ep + 2) % 4
    diag = (sib + 2) % 4
    to_sib, to_opp, to_tp = (dp, tp, sib), (dp, tp, opp), (dp, 1 - tp, ep)

    def gate_copies(f, slot):
        return (pltpu.make_async_copy(gate_hbm.at[f], ring.at[slot, :, pl.ds(0, width)], ring_sem.at[slot]),
                pltpu.make_async_copy(up_hbm.at[f], ring.at[slot, :, pl.ds(width, width)], ring_sem.at[slot]))

    def down_pieces(i):
        pieces, done = [], 0
        while done < width:
            at = i * width + done
            rows = min(width - done, d_model - at % d_model)
            pieces.append((done, rows, at % d_model, (at // d_model) * cols))
            done += rows
        return pieces

    def start_fill(f, slot):
        @pl.when(f < local)
        def _():
            for copy in gate_copies(f, slot):
                copy.start()

        @pl.when(jnp.logical_and(f >= local, f < fills))
        def _():
            h = f - local
            c, base = h // 2, (h % 2) * half
            col = pl.multiple_of(c * cols, cols)
            for i in range(half):
                for begin, rows, row, lane in down_pieces(i):
                    pltpu.make_async_copy(down_hbm.at[base + i, pl.ds(begin, rows), pl.ds(col, cols)],
                                          ring.at[slot, pl.ds(row, rows), pl.ds(lane, cols)], ring_sem.at[slot]).start()

    def wait_fill(slot):
        pltpu.make_async_copy(ring.at[slot], ring.at[slot], ring_sem.at[slot]).wait()

    own_x = pltpu.make_async_copy(x_hbm, xall.at[ep], load_sem.at[0])
    own_choice = pltpu.make_async_copy(choice_hbm, choice_t.at[ep], load_sem.at[1])
    own_scale = pltpu.make_async_copy(scale_hbm, scale_v, load_sem.at[2])
    own_router = pltpu.make_async_copy(router_hbm, router_v, load_sem.at[3])
    own_x.start()
    own_choice.start()
    own_scale.start()
    own_router.start()

    barrier = pltpu.get_barrier_semaphore()
    for peer in (to_sib, to_opp, to_tp):
        pl.semaphore_signal(barrier, inc=1, device_id=peer, device_id_type=MESH)
    for f in range(SLOTS):
        for copy in gate_copies(f, f):
            copy.start()

    def remote(src, dst, ssem, rsem, peer):
        return pltpu.make_async_remote_copy(src_ref=src, dst_ref=dst, send_sem=ssem, recv_sem=rsem, device_id=peer, device_id_type=MESH)

    mid = tok // 2
    piece = mid // HEAD_CHUNKS

    def rows_of(which, r):
        return pl.ds(pl.multiple_of(which * mid + r * piece, piece), piece)

    def same(block, rows, ssem, rsem, peer):
        return remote(xall.at[block, rows, :], xall.at[block, rows, :], ssem, rsem, peer)

    span = range(HEAD_CHUNKS)
    to_pair = remote(xall.at[ep], xall.at[ep], pair_send, pair_recv, to_sib)
    hops = [same(ep, rows_of(tp, r), hop_send.at[r], hop_recv.at[r], to_opp) for r in span]
    over = [same(opp, rows_of(tp, r), tp_send.at[r], tp_recv.at[r], to_tp) for r in span]
    near = [same(opp, rows_of(tp, r), near_send.at[r], near_recv.at[r], to_sib) for r in span]
    far = [same(opp, rows_of(1 - tp, r), far_send.at[r], far_recv.at[r], to_sib) for r in span]
    ch_pair = remote(choice_t.at[ep], choice_t.at[ep], ch_send.at[0], ch_recv.at[0], to_sib)
    ch_hop = remote(choice_t.at[ep], choice_t.at[ep], ch_send.at[1], ch_recv.at[1], to_opp)
    ch_fwd = remote(choice_t.at[opp], choice_t.at[opp], ch_send.at[2], ch_recv.at[2], to_sib)
    own_choice.wait()
    own_x.wait()
    pl.semaphore_wait(barrier, 3)
    ch_hop.start()
    for r in span:
        hops[r].start()
    ch_pair.start()
    to_pair.start()

    row_e = lax.broadcasted_iota(jnp.int32, (experts, tok), 0)
    earlier = (lax.broadcasted_iota(jnp.int32, (tok, tok), 0) < lax.broadcasted_iota(jnp.int32, (tok, tok), 1)).astype(BF16)
    slots = local * cap
    slot_row = lax.broadcasted_iota(jnp.int32, (slots, experts), 0)
    expand_t = (lax.broadcasted_iota(jnp.int32, (slots, experts), 1) == ep * local + slot_row // cap).astype(BF16)
    slot_col = lax.broadcasted_iota(jnp.int32, (experts, slots), 1)
    expand = (lax.broadcasted_iota(jnp.int32, (experts, slots), 0) == ep * local + slot_col // cap).astype(BF16)
    cap_row = (lax.broadcasted_iota(jnp.int32, (slots, tok), 0) % cap).astype(F32)
    cap_col = (lax.broadcasted_iota(jnp.int32, (tok, slots), 1) % cap).astype(F32)

    def positions(g):
        ids = choice_t[g]
        member = jnp.zeros((experts, tok), F32)
        for k in range(top_k):
            member = jnp.where(row_e == ids[k:k + 1, :], 1.0, member)
        before = jnp.dot(member.astype(BF16), earlier, preferred_element_type=F32)
        return member, jnp.where(member > 0.0, before, 255.0)

    def dispatch_table(g):
        member, place = positions(g)
        spot = jnp.dot(expand_t, place.astype(BF16), preferred_element_type=F32)
        disp[g] = (spot == cap_row).astype(BF16)

    def combine_table(g):
        member, place = positions(g)
        logits = jnp.dot(uall[g], router_v[...], preferred_element_type=F32)
        shifted = jnp.exp(logits - jnp.max(logits, axis=-1, keepdims=True))
        probs = shifted / jnp.sum(shifted, axis=-1, keepdims=True)
        picked = jnp.where(jnp.transpose(member) > 0.0, probs, 0.0)
        gates = picked / jnp.sum(picked, axis=-1, keepdims=True)
        spot = jnp.dot(jnp.transpose(place).astype(BF16), expand, preferred_element_type=F32)
        filled = spot == cap_col
        rest = gates
        for i in range(3):
            term = rest.astype(BF16)
            rest = rest - term.astype(F32)
            wide = jnp.dot(term, expand, preferred_element_type=F32)
            comb[g, pl.ds(i * tok, tok), :] = jnp.where(filled, wide, 0.0).astype(BF16)

    def normalize(g, first, rows):
        n = d_model // 128
        at = pl.ds(first, rows)
        scale = scale_v[...].astype(F32)
        total = jnp.zeros((rows, 128), F32)
        for j in range(n):
            total = total + xall[g, at, pl.ds(j * 128, 128)].astype(F32)
        mean = jnp.sum(total, axis=-1, keepdims=True) / d_model
        square = jnp.zeros((rows, 128), F32)
        for j in range(n):
            centered = xall[g, at, pl.ds(j * 128, 128)].astype(F32) - mean
            square = square + centered * centered
        inv = lax.rsqrt(jnp.sum(square, axis=-1, keepdims=True) / d_model + NORM_EPS)
        for j in range(n):
            centered = xall[g, at, pl.ds(j * 128, 128)].astype(F32) - mean
            uall[g, at, pl.ds(j * 128, 128)] = (centered * inv * scale[j:j + 1, :]).astype(BF16)

    here, there = pl.multiple_of(tp * mid, mid), pl.multiple_of((1 - tp) * mid, mid)
    own_scale.wait()
    normalize(ep, 0, tok)
    dispatch_table(ep)
    ch_pair.wait_recv()
    to_pair.wait_recv()
    normalize(sib, 0, tok)
    dispatch_table(sib)
    own_router.wait()
    combine_table(ep)

    def pass_hop(r):
        hops[r].wait_recv()
        over[r].start()
        near[r].start()

    def pass_over(r):
        over[r].wait_recv()
        far[r].start()

    ch_hop.wait_recv()
    ch_fwd.start()
    lead = 4
    for r in range(lead):
        pass_hop(r)
    combine_table(sib)
    dispatch_table(opp)
    ch_fwd.wait_recv()
    dispatch_table(diag)
    for r in range(lead, HEAD_CHUNKS):
        pass_hop(r)
        pass_over(r - lead)
    normalize(opp, here, mid)
    for r in range(HEAD_CHUNKS - lead, HEAD_CHUNKS):
        pass_over(r)
    for r in span:
        near[r].wait_recv()
    normalize(diag, here, mid)
    normalize(opp, there, mid)
    for r in span:
        far[r].wait_recv()
    normalize(diag, there, mid)

    def steady(rows, weight):
        twice = jnp.dot(jnp.concatenate([rows, rows], axis=0), weight, preferred_element_type=F32)
        return jnp.minimum(twice[:rows.shape[0]], twice[rows.shape[0]:])

    batch = tok // cap
    wide = 512

    def first_products(b, refill_each):
        for g in range(groups):
            table = disp[g, pl.ds(pl.multiple_of(b * tok, tok), tok), :]
            for j in range(d_model // wide):
                xbatch[g, :, pl.ds(j * wide, wide)] = jnp.dot(table, uall[g, :, pl.ds(j * wide, wide)], preferred_element_type=F32).astype(BF16)

        @pl.when(jnp.logical_and(b >= 1, b < 3))
        def _():
            combine_table(jnp.where(b == 1, opp, diag))

        @pl.loop(0, batch // UNROLL)
        def _(i):
            first = b * batch + i * UNROLL
            for k in range(UNROLL):
                wait_fill((first + k) % SLOTS)
            for k in range(UNROLL):
                slot = (first + k) % SLOTS
                row = pl.multiple_of((i * UNROLL + k) * cap, cap)
                rows = jnp.concatenate([xbatch[g, pl.ds(row, cap), :] for g in range(groups)], axis=0)
                both = steady(rows, ring[slot])
                if refill_each:
                    for copy in gate_copies(first + k + SLOTS, slot):
                        copy.start()
                hid[first + k] = (jax.nn.silu(both[:, :width]) * both[:, width:]).astype(BF16)
            if not refill_each:
                for k in range(UNROLL):
                    start_fill(first + k + SLOTS, (first + k) % SLOTS)

    early = (local - SLOTS) // batch

    @pl.loop(0, early)
    def _(b):
        first_products(b, True)

    @pl.loop(early, local // batch)
    def _(b):
        first_products(b, False)

    def pair_copy(c, j):
        return remote(pair_out.at[c % PAIR_SLOTS, j], pair_in.at[c, j], p_send.at[c, j], p_recv.at[c, j], to_sib)

    def at_cols(c):
        return pl.ds(pl.multiple_of(c * cols, cols), cols)

    halves = range(cols // 128)

    def at_half(c, t):
        return pl.ds(pl.multiple_of(c * cols + t * 128, 128), 128)

    def x_copy(c, t):
        return remote(xbatch.at[0, :, at_half(c, t)], row_in.at[c, t], x_send.at[c, t], x_recv.at[c, t], to_opp)

    def y_copy(c, t):
        return remote(xbatch.at[1, :, at_half(c, t)], col_in.at[c, t], y_send.at[c, t], y_recv.at[c, t], to_tp)

    def out_copy(c):
        return pltpu.make_async_copy(xbatch.at[2, :, at_cols(c)], out_hbm.at[:, at_cols(c)], out_sem.at[c])

    def half_products(c, h):
        f = local + 2 * c + h
        slot = f % SLOTS
        wait_fill(slot)
        for i in range(half):
            e = h * half + i
            parts = [ring[slot, pl.ds(row, rows), pl.ds(lane, cols)] for begin, rows, row, lane in down_pieces(i)]
            weight = parts[0] if len(parts) == 1 else jnp.concatenate(parts, axis=0)
            q = jnp.dot(hid[e], weight, preferred_element_type=F32).astype(BF16)
            for g in range(groups):
                qbuf[g, pl.ds(e * cap, cap), :] = q[g * cap:(g + 1) * cap, :]
        start_fill(f + SLOTS, slot)

    def weighted(g):
        terms = jnp.dot(comb[g], qbuf[g], preferred_element_type=F32)
        return terms[0:tok] + terms[tok:2 * tok] + terms[2 * tok:3 * tok]

    def sums(c):
        @pl.when(c >= PAIR_SLOTS)
        def _():
            for j in range(2):
                pair_copy(c - PAIR_SLOTS, j).wait_send()

        for j in (1 - side, side):
            pair_out[c % PAIR_SLOTS, j] = weighted(2 * j + 1 - core)
            pair_copy(c, j).start()
        for j in range(2):
            part[c, j] = weighted(2 * j + core)

    def send_x(c):
        pair_copy(c, 1 - side).wait_recv()
        for t in halves:
            at = pl.ds(t * 128, 128)
            xbatch[0, :, at_half(c, t)] = (part[c, 1 - side, :, at] + pair_in[c, 1 - side, :, at]).astype(BF16)
            x_copy(c, t).start()
        pair_copy(c, side).wait_recv()
        part[c, side] = part[c, side] + pair_in[c, side]

    def send_y(c):
        for t in halves:
            x_copy(c, t).wait_recv()
            xbatch[1, :, at_half(c, t)] = (part[c, side, :, pl.ds(t * 128, 128)] + row_in[c, t].astype(F32)).astype(BF16)
            y_copy(c, t).start()

    def finish(c):
        for t in halves:
            y_copy(c, t).wait_recv()
            total = xbatch[1, :, at_half(c, t)].astype(F32) + col_in[c, t].astype(F32)
            xbatch[2, :, at_half(c, t)] = (xall[ep, :, at_half(c, t)].astype(F32) + total).astype(BF16)
        out_copy(c).start()

    @pl.loop(0, chunks + LAG_OUT)
    def _(c):
        @pl.when(c < chunks)
        def _():
            half_products(c, 0)
            half_products(c, 1)

        for lag, stage in ((LAG_X, send_x), (LAG_Y, send_y), (LAG_OUT, finish)):
            @pl.when(jnp.logical_and(c >= lag, c < chunks + lag))
            def _():
                stage(c - lag)

        @pl.when(c < chunks)
        def _():
            sums(c)

    to_pair.wait_send()
    for copies in (hops, over, near, far):
        for r in span:
            copies[r].wait_send()
    ch_pair.wait_send()
    ch_hop.wait_send()
    ch_fwd.wait_send()

    @pl.loop(chunks - PAIR_SLOTS, chunks)
    def _(c):
        for j in range(2):
            pair_copy(c, j).wait_send()

    @pl.loop(0, chunks)
    def _(c):
        for t in halves:
            x_copy(c, t).wait_send()
            y_copy(c, t).wait_send()
        out_copy(c).wait()


def solution(mesh):
    row_spec = P(('dp', 'ep'), None)

    def device_step(resid_in, norm_scale, w_router, w_gate, w_up, w_down, choice):
        tok, d_model = resid_in.shape
        experts, top_k = w_router.shape[1], choice.shape[1]
        local, width = w_gate.shape[0], w_gate.shape[2]
        groups = experts // local
        cap = (2 * tok * top_k + experts - 1) // experts
        cols = 256
        chunks = d_model // cols
        dims = (tok, d_model, experts, top_k, local, width, groups, cap, cols)
        dma = pltpu.SemaphoreType.DMA
        vmem = pltpu.VMEM
        return pl.pallas_call(
            functools.partial(moe_kernel, dims),
            out_shape=jax.ShapeDtypeStruct((tok, d_model), BF16),
            in_specs=[pl.BlockSpec(memory_space=pl.ANY)] * 7,
            out_specs=pl.BlockSpec(memory_space=pl.ANY),
            scratch_shapes=[
                vmem((SLOTS, d_model, 2 * width), BF16),
                vmem((groups, tok, d_model), BF16),
                vmem((groups, tok, d_model), BF16),
                vmem((groups, tok, d_model), BF16),
                vmem((local, groups * cap, width), BF16),
                vmem((groups, local * cap, tok), BF16),
                vmem((groups, 3 * tok, local * cap), BF16),
                vmem((groups, local * cap, cols), BF16),
                vmem((chunks, 2, tok, cols), F32),
                vmem((PAIR_SLOTS, 2, tok, cols), F32),
                vmem((chunks, 2, tok, cols), F32),
                *[vmem((chunks, cols // 128, tok, 128), BF16) for _ in range(2)],
                vmem((d_model // 128, 128), BF16),
                vmem((d_model, experts), BF16),
                vmem((groups, top_k, tok), jnp.int32),
                dma((SLOTS,)), dma((4,)), dma(()), dma(()),
                *[dma((HEAD_CHUNKS,)) for _ in range(8)],
                dma((3,)), dma((3,)),
                dma((chunks, 2)), dma((chunks, 2)),
                *[dma((chunks, cols // 128)) for _ in range(4)],
                dma((chunks,)),
            ],
            compiler_params=pltpu.CompilerParams(collective_id=0, has_side_effects=True, vmem_limit_bytes=67043328),
        )(resid_in, norm_scale.reshape(d_model // 128, 128), w_router, w_gate, w_up, w_down, choice.T)

    return jax.shard_map(device_step, mesh=mesh, in_specs=(row_spec, P(None), P(None, None), P('ep', None, 'tp'), P('ep', None, 'tp'), P('ep', 'tp', None), row_spec), out_specs=row_spec, check_vma=False)
```

```python
import functools

import jax
import jax.numpy as jnp
from jax import lax
from jax.experimental import pallas as pl
from jax.experimental.pallas import tpu as pltpu
from jax.sharding import PartitionSpec as P

NORM_EPS = 1e-5
MESH = pl.DeviceIdType.MESH
F32 = jnp.float32
BF16 = jnp.bfloat16

SLOTS = 15
PAIR_SLOTS = 1
UNROLL = 4
HEAD_CHUNKS = 8
LAG_X = 1
LAG_Y = 3
LAG_OUT = 5


def moe_kernel(dims, x_hbm, scale_hbm, router_hbm, gate_hbm, up_hbm, down_hbm, choice_hbm, out_hbm,
               ring, xall, uall, xbatch, hid, comb, qbuf, part, far_sum, pair_out, pair_in, row_in, col_in,
               scale_v, router_v, choice_t, ring_sem, load_sem, pair_send, pair_recv, hop_send, hop_recv, tp_send, tp_recv,
               near_send, near_recv, far_send, far_recv, ch_send, ch_recv, p_send, p_recv, x_send, x_recv, y_send, y_recv, out_sem):
    tok, d_model, experts, top_k, local, width, groups, cap, cols = dims
    chunks = d_model // cols
    half = local // 2
    fills = local + 2 * chunks
    ep = lax.axis_index('ep')
    tp = lax.axis_index('tp')
    dp = lax.axis_index('dp')
    core, side = ep % 2, ep // 2
    sib = ep + 1 - 2 * core
    opp = (ep + 2) % 4
    diag = (sib + 2) % 4
    to_sib, to_opp, to_tp = (dp, tp, sib), (dp, tp, opp), (dp, 1 - tp, ep)

    def gate_copies(f, slot):
        return (pltpu.make_async_copy(gate_hbm.at[f], ring.at[slot, :, pl.ds(0, width)], ring_sem.at[slot]),
                pltpu.make_async_copy(up_hbm.at[f], ring.at[slot, :, pl.ds(width, width)], ring_sem.at[slot]))

    def down_pieces(i):
        pieces, done = [], 0
        while done < width:
            at = i * width + done
            rows = min(width - done, d_model - at % d_model)
            pieces.append((done, rows, at % d_model, (at // d_model) * cols))
            done += rows
        return pieces

    def start_fill(f, slot):
        @pl.when(f < local)
        def _():
            for copy in gate_copies(f, slot):
                copy.start()

        @pl.when(jnp.logical_and(f >= local, f < fills))
        def _():
            h = f - local
            c, base = h // 2, (h % 2) * half
            col = pl.multiple_of(c * cols, cols)
            for i in range(half):
                for begin, rows, row, lane in down_pieces(i):
                    pltpu.make_async_copy(down_hbm.at[base + i, pl.ds(begin, rows), pl.ds(col, cols)],
                                          ring.at[slot, pl.ds(row, rows), pl.ds(lane, cols)], ring_sem.at[slot]).start()

    def wait_fill(slot):
        pltpu.make_async_copy(ring.at[slot], ring.at[slot], ring_sem.at[slot]).wait()

    own_x = pltpu.make_async_copy(x_hbm, xall.at[ep], load_sem.at[0])
    own_choice = pltpu.make_async_copy(choice_hbm, choice_t.at[ep], load_sem.at[1])
    own_scale = pltpu.make_async_copy(scale_hbm, scale_v, load_sem.at[2])
    own_router = pltpu.make_async_copy(router_hbm, router_v, load_sem.at[3])
    own_x.start()
    own_choice.start()
    own_scale.start()
    own_router.start()

    barrier = pltpu.get_barrier_semaphore()
    for peer in (to_sib, to_opp, to_tp):
        pl.semaphore_signal(barrier, inc=1, device_id=peer, device_id_type=MESH)
    for f in range(SLOTS):
        for copy in gate_copies(f, f):
            copy.start()

    def remote(src, dst, ssem, rsem, peer):
        return pltpu.make_async_remote_copy(src_ref=src, dst_ref=dst, send_sem=ssem, recv_sem=rsem, device_id=peer, device_id_type=MESH)

    mid = tok // 2
    piece = mid // HEAD_CHUNKS

    def rows_of(which, r):
        return pl.ds(pl.multiple_of(which * mid + r * piece, piece), piece)

    def same(block, rows, ssem, rsem, peer):
        return remote(xall.at[block, rows, :], xall.at[block, rows, :], ssem, rsem, peer)

    span = range(HEAD_CHUNKS)
    to_pair = remote(xall.at[ep], xall.at[ep], pair_send, pair_recv, to_sib)
    hops = [same(ep, rows_of(tp, r), hop_send.at[r], hop_recv.at[r], to_opp) for r in span]
    over = [same(opp, rows_of(tp, r), tp_send.at[r], tp_recv.at[r], to_tp) for r in span]
    near = [same(opp, rows_of(tp, r), near_send.at[r], near_recv.at[r], to_sib) for r in span]
    far = [same(opp, rows_of(1 - tp, r), far_send.at[r], far_recv.at[r], to_sib) for r in span]
    ch_pair = remote(choice_t.at[ep], choice_t.at[ep], ch_send.at[0], ch_recv.at[0], to_sib)
    ch_hop = remote(choice_t.at[ep], choice_t.at[ep], ch_send.at[1], ch_recv.at[1], to_opp)
    ch_fwd = remote(choice_t.at[opp], choice_t.at[opp], ch_send.at[2], ch_recv.at[2], to_sib)
    own_choice.wait()
    own_x.wait()
    pl.semaphore_wait(barrier, 3)
    ch_hop.start()
    for r in span:
        hops[r].start()
    ch_pair.start()
    to_pair.start()

    row_e = lax.broadcasted_iota(jnp.int32, (experts, tok), 0)
    earlier = (lax.broadcasted_iota(jnp.int32, (tok, tok), 0) < lax.broadcasted_iota(jnp.int32, (tok, tok), 1)).astype(BF16)
    slots = local * cap
    slot_row = lax.broadcasted_iota(jnp.int32, (slots, experts), 0)
    expand_t = (lax.broadcasted_iota(jnp.int32, (slots, experts), 1) == ep * local + slot_row // cap).astype(BF16)
    slot_col = lax.broadcasted_iota(jnp.int32, (experts, slots), 1)
    expand = (lax.broadcasted_iota(jnp.int32, (experts, slots), 0) == ep * local + slot_col // cap).astype(BF16)
    cap_row = (lax.broadcasted_iota(jnp.int32, (slots, tok), 0) % cap).astype(F32)
    cap_col = (lax.broadcasted_iota(jnp.int32, (tok, slots), 1) % cap).astype(F32)

    def positions(g):
        ids = choice_t[g]
        member = jnp.zeros((experts, tok), F32)
        for k in range(top_k):
            member = jnp.where(row_e == ids[k:k + 1, :], 1.0, member)
        before = jnp.dot(member.astype(BF16), earlier, preferred_element_type=F32)
        return member, jnp.where(member > 0.0, before, 255.0)

    def dispatch_table(g):
        member, place = positions(g)
        spot = jnp.dot(expand_t, place.astype(BF16), preferred_element_type=F32)
        qbuf[g, :, pl.ds(0, tok)] = (spot == cap_row).astype(BF16)

    def combine_table(g):
        member, place = positions(g)
        logits = jnp.dot(uall[g], router_v[...], preferred_element_type=F32)
        shifted = jnp.exp(logits - jnp.max(logits, axis=-1, keepdims=True))
        probs = shifted / jnp.sum(shifted, axis=-1, keepdims=True)
        picked = jnp.where(jnp.transpose(member) > 0.0, probs, 0.0)
        gates = picked / jnp.sum(picked, axis=-1, keepdims=True)
        spot = jnp.dot(jnp.transpose(place).astype(BF16), expand, preferred_element_type=F32)
        filled = spot == cap_col
        rest = gates
        for i in range(3):
            term = rest.astype(BF16)
            rest = rest - term.astype(F32)
            wide = jnp.dot(term, expand, preferred_element_type=F32)
            comb[g, pl.ds(i * tok, tok), :] = jnp.where(filled, wide, 0.0).astype(BF16)

    def normalize(g, first, rows):
        n = d_model // 128
        at = pl.ds(first, rows)
        scale = scale_v[...].astype(F32)
        total = jnp.zeros((rows, 128), F32)
        for j in range(n):
            total = total + xall[g, at, pl.ds(j * 128, 128)].astype(F32)
        mean = jnp.sum(total, axis=-1, keepdims=True) / d_model
        square = jnp.zeros((rows, 128), F32)
        for j in range(n):
            centered = xall[g, at, pl.ds(j * 128, 128)].astype(F32) - mean
            square = square + centered * centered
        inv = lax.rsqrt(jnp.sum(square, axis=-1, keepdims=True) / d_model + NORM_EPS)
        for j in range(n):
            centered = xall[g, at, pl.ds(j * 128, 128)].astype(F32) - mean
            uall[g, at, pl.ds(j * 128, 128)] = (centered * inv * scale[j:j + 1, :]).astype(BF16)

    here, there = pl.multiple_of(tp * mid, mid), pl.multiple_of((1 - tp) * mid, mid)
    own_scale.wait()
    normalize(ep, 0, tok)
    dispatch_table(ep)
    ch_pair.wait_recv()
    to_pair.wait_recv()
    normalize(sib, 0, tok)
    dispatch_table(sib)
    own_router.wait()
    combine_table(ep)

    def pass_hop(r):
        hops[r].wait_recv()
        over[r].start()
        near[r].start()

    def pass_over(r):
        over[r].wait_recv()
        far[r].start()

    ch_hop.wait_recv()
    ch_fwd.start()
    lead = 4
    for r in range(lead):
        pass_hop(r)
    combine_table(sib)
    dispatch_table(opp)
    ch_fwd.wait_recv()
    dispatch_table(diag)
    for r in range(lead, HEAD_CHUNKS):
        pass_hop(r)
        pass_over(r - lead)
    normalize(opp, here, mid)
    for r in range(HEAD_CHUNKS - lead, HEAD_CHUNKS):
        pass_over(r)
    for r in span:
        near[r].wait_recv()
    normalize(diag, here, mid)
    normalize(opp, there, mid)
    for r in span:
        far[r].wait_recv()
    normalize(diag, there, mid)

    def steady(rows, weight):
        twice = jnp.dot(jnp.concatenate([rows, rows], axis=0), weight, preferred_element_type=F32)
        return jnp.minimum(twice[:rows.shape[0]], twice[rows.shape[0]:])

    batch = tok // cap
    wide = 512

    def first_products(b, refill_each):
        for g in range(groups):
            table = qbuf[g, pl.ds(pl.multiple_of(b * tok, tok), tok), pl.ds(0, tok)]
            for j in range(d_model // wide):
                xbatch[g, :, pl.ds(j * wide, wide)] = jnp.dot(table, uall[g, :, pl.ds(j * wide, wide)], preferred_element_type=F32).astype(BF16)

        @pl.when(jnp.logical_and(b >= 1, b < 3))
        def _():
            combine_table(jnp.where(b == 1, opp, diag))

        @pl.loop(0, batch // UNROLL)
        def _(i):
            first = b * batch + i * UNROLL
            for k in range(UNROLL):
                wait_fill((first + k) % SLOTS)
            for k in range(UNROLL):
                slot = (first + k) % SLOTS
                row = pl.multiple_of((i * UNROLL + k) * cap, cap)
                rows = jnp.concatenate([xbatch[g, pl.ds(row, cap), :] for g in range(groups)], axis=0)
                both = steady(rows, ring[slot])
                if refill_each:
                    for copy in gate_copies(first + k + SLOTS, slot):
                        copy.start()
                hid[first + k] = (jax.nn.silu(both[:, :width]) * both[:, width:]).astype(BF16)
            if not refill_each:
                for k in range(UNROLL):
                    start_fill(first + k + SLOTS, (first + k) % SLOTS)

    early = (local - SLOTS) // batch

    @pl.loop(0, early)
    def _(b):
        first_products(b, True)

    @pl.loop(early, local // batch)
    def _(b):
        first_products(b, False)

    def pair_copy(c, j):
        return remote(pair_out.at[c % PAIR_SLOTS, j], pair_in.at[c, j], p_send.at[c, j], p_recv.at[c, j], to_sib)

    def at_cols(c):
        return pl.ds(pl.multiple_of(c * cols, cols), cols)

    halves = range(cols // 128)

    def at_half(c, t):
        return pl.ds(pl.multiple_of(c * cols + t * 128, 128), 128)

    def x_copy(c, t):
        return remote(xbatch.at[0, :, at_half(c, t)], row_in.at[c, t], x_send.at[c, t], x_recv.at[c, t], to_opp)

    def y_copy(c, t):
        return remote(xbatch.at[1, :, at_half(c, t)], col_in.at[c, t], y_send.at[c, t], y_recv.at[c, t], to_tp)

    def out_copy(c):
        return pltpu.make_async_copy(xbatch.at[2, :, at_cols(c)], out_hbm.at[:, at_cols(c)], out_sem.at[c])

    def half_products(c, h):
        f = local + 2 * c + h
        slot = f % SLOTS
        wait_fill(slot)
        for i in range(half):
            e = h * half + i
            parts = [ring[slot, pl.ds(row, rows), pl.ds(lane, cols)] for begin, rows, row, lane in down_pieces(i)]
            weight = parts[0] if len(parts) == 1 else jnp.concatenate(parts, axis=0)
            q = jnp.dot(hid[e], weight, preferred_element_type=F32).astype(BF16)
            for g in range(groups):
                qbuf[g, pl.ds(e * cap, cap), :] = q[g * cap:(g + 1) * cap, :]
        start_fill(f + SLOTS, slot)

    def weighted(g):
        terms = jnp.dot(comb[g], qbuf[g], preferred_element_type=F32)
        return terms[0:tok] + terms[tok:2 * tok] + terms[2 * tok:3 * tok]

    def sums(c):
        @pl.when(c >= PAIR_SLOTS)
        def _():
            for j in range(2):
                pair_copy(c - PAIR_SLOTS, j).wait_send()

        for j in (1 - side, side):
            pair_out[c % PAIR_SLOTS, j] = weighted(2 * j + 1 - core)
            pair_copy(c, j).start()
        far_sum[...] = weighted(2 * (1 - side) + core)
        part[c] = weighted(2 * side + core)

    def send_x(c):
        pair_copy(c, 1 - side).wait_recv()
        for t in halves:
            at = pl.ds(t * 128, 128)
            xbatch[0, :, at_half(c, t)] = (far_sum[:, at] + pair_in[c, 1 - side, :, at]).astype(BF16)
            x_copy(c, t).start()
        pair_copy(c, side).wait_recv()
        part[c] = part[c] + pair_in[c, side]

    def send_y(c):
        for t in halves:
            x_copy(c, t).wait_recv()
            xbatch[1, :, at_half(c, t)] = (part[c, :, pl.ds(t * 128, 128)] + row_in[c, t].astype(F32)).astype(BF16)
            y_copy(c, t).start()

    def finish(c):
        for t in halves:
            y_copy(c, t).wait_recv()
            total = xbatch[1, :, at_half(c, t)].astype(F32) + col_in[c, t].astype(F32)
            xbatch[2, :, at_half(c, t)] = (xall[ep, :, at_half(c, t)].astype(F32) + total).astype(BF16)
        out_copy(c).start()

    @pl.loop(0, chunks + LAG_OUT)
    def _(c):
        @pl.when(c < chunks)
        def _():
            half_products(c, 0)
            half_products(c, 1)

        for lag, stage in ((LAG_X, send_x), (LAG_Y, send_y), (LAG_OUT, finish)):
            @pl.when(jnp.logical_and(c >= lag, c < chunks + lag))
            def _():
                stage(c - lag)

        @pl.when(c < chunks)
        def _():
            sums(c)

    to_pair.wait_send()
    for copies in (hops, over, near, far):
        for r in span:
            copies[r].wait_send()
    ch_pair.wait_send()
    ch_hop.wait_send()
    ch_fwd.wait_send()

    @pl.loop(chunks - PAIR_SLOTS, chunks)
    def _(c):
        for j in range(2):
            pair_copy(c, j).wait_send()

    @pl.loop(0, chunks)
    def _(c):
        for t in halves:
            x_copy(c, t).wait_send()
            y_copy(c, t).wait_send()
        out_copy(c).wait()


def solution(mesh):
    row_spec = P(('dp', 'ep'), None)

    def device_step(resid_in, norm_scale, w_router, w_gate, w_up, w_down, choice):
        tok, d_model = resid_in.shape
        experts, top_k = w_router.shape[1], choice.shape[1]
        local, width = w_gate.shape[0], w_gate.shape[2]
        groups = experts // local
        cap = (2 * tok * top_k + experts - 1) // experts
        cols = 256
        chunks = d_model // cols
        dims = (tok, d_model, experts, top_k, local, width, groups, cap, cols)
        dma = pltpu.SemaphoreType.DMA
        vmem = pltpu.VMEM
        return pl.pallas_call(
            functools.partial(moe_kernel, dims),
            out_shape=jax.ShapeDtypeStruct((tok, d_model), BF16),
            in_specs=[pl.BlockSpec(memory_space=pl.ANY)] * 7,
            out_specs=pl.BlockSpec(memory_space=pl.ANY),
            scratch_shapes=[
                vmem((SLOTS, d_model, 2 * width), BF16),
                vmem((groups, tok, d_model), BF16),
                vmem((groups, tok, d_model), BF16),
                vmem((groups, tok, d_model), BF16),
                vmem((local, groups * cap, width), BF16),
                vmem((groups, 3 * tok, local * cap), BF16),
                vmem((groups, local * cap, cols), BF16),
                vmem((chunks, tok, cols), F32),
                vmem((tok, cols), F32),
                vmem((PAIR_SLOTS, 2, tok, cols), F32),
                vmem((chunks, 2, tok, cols), F32),
                *[vmem((chunks, cols // 128, tok, 128), BF16) for _ in range(2)],
                vmem((d_model // 128, 128), BF16),
                vmem((d_model, experts), BF16),
                vmem((groups, top_k, tok), jnp.int32),
                dma((SLOTS,)), dma((4,)), dma(()), dma(()),
                *[dma((HEAD_CHUNKS,)) for _ in range(8)],
                dma((3,)), dma((3,)),
                dma((chunks, 2)), dma((chunks, 2)),
                *[dma((chunks, cols // 128)) for _ in range(4)],
                dma((chunks,)),
            ],
            compiler_params=pltpu.CompilerParams(collective_id=0, has_side_effects=True, vmem_limit_bytes=67043328),
        )(resid_in, norm_scale.reshape(d_model // 128, 128), w_router, w_gate, w_up, w_down, choice.T)

    return jax.shard_map(device_step, mesh=mesh, in_specs=(row_spec, P(None), P(None, None), P('ep', None, 'tp'), P('ep', None, 'tp'), P('ep', 'tp', None), row_spec), out_specs=row_spec, check_vma=False)
```
